32 devices in a mesh: groups: 1, ep: 32 (over z, y, x, core).
Axes of the slice: x: 2, y: 2, z: 4, core: 2. Of those that a mesh axis runs over, the one named last changes fastest.
Arguments:
- tokens: bfloat16 [2048, 2880], P(('groups', 'ep')), may hold values from -6 to 6
- routes: int32 [2048, 4], P(('groups', 'ep')), may hold values from 0 to 7, all different within a row; in each aligned block of 64 rows (0 to 63, 64 to 127, ...) at most 36 rows name the same one
- norm_gain: bfloat16 [2880], replicated, may hold values from 0.25 to 1.75
- router_weight: bfloat16 [2880, 8], replicated, may hold values from -0.02734375 to 0.02734375
- gate_up_weight: bfloat16 [32, 2880, 720], P('ep'), may hold values from -0.109375 to 0.109375
- down_weight: bfloat16 [32, 360, 2880], P('ep'), may hold values from -0.15625 to 0.15625
Outputs:
- mixed: bfloat16 [2048, 2880], P(('groups', 'ep'))
The draws below stay inside these ranges and needn't reach their ends.
Inputs may be any that keep to these rules, and one draw needn't show every extreme that they name: `routes`: in each aligned block of 64 rows (the rows of one device), no expert is named by more than 36 rows; in some blocks one expert is named by exactly 36 rows. A row names 4 different experts.
All inputs are finite; a program needn't handle non-finite values.
Results may differ from the reference program's by a relative error of at most 0.005.
Values may be sent and summed in bfloat16 or wider, within the bound.
A program may use at most 128 MiB of HBM per device.

```python
import math
import jax
import jax.numpy as jnp
import numpy as np
from jax import lax

D = 2880
FF_WIN = 1440
TOP = 4
SHARD = 4
TOK_DEV = 64
EXPERTS = 8
FF_DEV = 360
CAP = 36
TOKENS = 2048
N_EP = 32


def level_of(own_key, extent, pieces, least, high):
    def one(axis_at, shards_of):
        steps = jax.random.uniform(jax.random.fold_in(jax.random.fold_in(own_key, 6), axis_at), (shards_of,), jnp.float32, least / len(pieces), high / len(pieces))
        return jnp.repeat(jnp.exp(steps), extent[axis_at] // shards_of).reshape((-1,) + (1,) * (len(extent) - axis_at - 1))

    level = one(*pieces[0])
    for cut in pieces[1:]:
        level = level * one(*cut)
    return level


def assign_block(own_key, own, number, rows, number_of, top, reach, slope):
    order = jax.random.permutation(own_key, number_of)
    heavy_load, usual = load_shares(number_of, rows * top, reach, slope, True), load_shares(number_of, rows * top, reach, slope, False)
    places = jnp.arange(number_of)

    def named(lengths, turn):
        used = int((lengths > 0).sum())
        fixed = max(1, used // 4)
        shifted = fixed + (places - fixed + turn * (used - fixed)) % max(1, number_of - fixed)
        return jnp.zeros((number_of,), jnp.int32).at[order[jnp.where(places < fixed, places, shifted)]].set(jnp.asarray(lengths, jnp.int32))

    lengths = jnp.where(number % 4 == 0, named(heavy_load, number // 4), named(usual, number - number // 4 - 1))
    mixed = jax.random.permutation(jax.random.fold_in(own, 3), number_of)
    source_of, receiver = mixed[0:number_of // 2 * 2:2], mixed[1:number_of // 2 * 2:2]
    margin = jnp.minimum(lengths[source_of] - 1, reach - lengths[receiver]) // 2
    margin = jnp.where((source_of == order[0]) | (receiver == order[0]) | (lengths[receiver] == 0), 0, jnp.maximum(margin, 0))
    shifted = jax.random.randint(jax.random.fold_in(own, 4), (number_of // 2,), 0, 1 << 20) % (margin + 1)
    lengths = lengths.at[source_of].add(-shifted).at[receiver].add(shifted)
    members = jnp.searchsorted(jnp.cumsum(lengths), jnp.arange(rows * top), side="right").astype(jnp.int32)
    table = members.reshape(top, rows).T
    table = table[jax.random.permutation(jax.random.fold_in(own, 1), rows)]
    turn = jax.random.randint(jax.random.fold_in(own, 2), (rows, 1), 0, top)
    return jnp.take_along_axis(table, (jnp.arange(top)[None, :] + turn) % top, axis=1)


def load_shares(number_of, total, reach, lean, full):
    portions = [(1 << 20) // math.isqrt(standing ** lean) + 1 for standing in range(1, number_of + 1)]
    largest = reach if full else min(reach, max(-(-total // number_of), total * portions[0] // sum(portions)))
    least = 1 if total - largest >= number_of - 1 else 0
    given, rest = [largest] + [least] * (number_of - 1), total - largest - least * (number_of - 1)
    while rest > 0:
        free = [i for i in range(1, number_of) if given[i] < largest] or [i for i in range(1, number_of) if given[i] < reach]
        whole, left = sum([portions[i] for i in free]), rest
        for i in free:
            more = min(reach - given[i], max(1, left * portions[i] // whole), rest)
            given[i] = given[i] + more
            rest = rest - more
    return np.array(given)


def centred(stream_key, shape, width, reach, cuts=(), held_as=jnp.bfloat16):
    values = width * jax.random.normal(stream_key, shape, jnp.float32)
    if cuts:
        values = values * level_of(stream_key, shape, cuts, -0.22, 0.18)
    return jnp.clip(values, -reach, reach).astype(held_as)


def setup_inputs(seed: int = 0, part: int = 0) -> dict:
    streams_of = jax.random.split(jax.random.key(seed), 7)
    own_keys = jax.random.split(jax.random.fold_in(streams_of[6], part), 7)
    tokens = centred(own_keys[0], (TOKENS, D), 1.0, 6.0, ((0, 32),))
    routes_keys = jax.random.split(jax.random.fold_in(own_keys[1], 1), TOKENS // TOK_DEV)
    routes_turns = jax.random.permutation(jax.random.fold_in(own_keys[1], 3), TOKENS // TOK_DEV)
    routes = jax.vmap(lambda own, number: assign_block(jax.random.fold_in(own_keys[1], 2), own, number, TOK_DEV, EXPERTS, TOP, CAP, 2))(routes_keys, routes_turns).reshape((TOKENS, TOP))
    norm_gain = jnp.clip(1.0 + 0.15 * jax.random.normal(streams_of[2], (D,), jnp.float32), 0.25, 1.75).astype(jnp.bfloat16)
    router_weight = centred(streams_of[3], (D, EXPERTS), (16 * D) ** -0.5, 0.02734375)
    gate_up_weight = centred(streams_of[4], (EXPERTS * SHARD, D, 2 * FF_DEV), D ** -0.5, 0.109375, ((0, 32),))
    down_weight = centred(streams_of[5], (EXPERTS * SHARD, FF_DEV, D), FF_WIN ** -0.5, 0.15625, ((0, 32),))
    return dict(tokens=tokens, routes=routes, norm_gain=norm_gain, router_weight=router_weight, gate_up_weight=gate_up_weight, down_weight=down_weight)


def reference(tokens, routes, norm_gain, router_weight, gate_up_weight, down_weight):
    stream = tokens.astype(jnp.float32)
    mean_square = lax.optimization_barrier(jnp.mean(stream * stream, axis=-1, keepdims=True))
    normed = (stream * lax.rsqrt(mean_square + 1e-05) * norm_gain.astype(jnp.float32)).astype(jnp.bfloat16)
    logits = jnp.dot(normed, router_weight, preferred_element_type=jnp.float32)
    expert_ids = jnp.arange(EXPERTS, dtype=jnp.int32)
    onehot = routes[:, :, None] == expert_ids[None, None, :]
    chosen = lax.optimization_barrier(jnp.sum(jnp.where(onehot, logits[:, None, :], jnp.float32(0.0)), axis=-1))
    expo = jnp.exp(chosen)
    route_prob = expo / lax.optimization_barrier(jnp.sum(expo, axis=-1, keepdims=True))
    flat_hits = onehot.astype(jnp.int32).reshape(N_EP, TOK_DEV * TOP, EXPERTS)
    rank_before = jnp.cumsum(flat_hits, axis=1) - flat_hits
    slot_index = lax.optimization_barrier(jnp.sum(flat_hits * rank_before, axis=-1)).reshape(TOKENS, TOP).astype(jnp.int32)
    block_ids = (jnp.arange(TOKENS, dtype=jnp.int32) // TOK_DEV)[:, None]
    position = (block_ids * CAP + slot_index).astype(jnp.int32)
    values = jnp.broadcast_to(normed[:, None, :], (TOKENS, TOP, D))
    buffer = jnp.zeros((EXPERTS, N_EP * CAP, D), jnp.bfloat16).at[routes, position].set(values)
    gate_up_all = gate_up_weight.reshape(EXPERTS, SHARD, D, 2 * FF_DEV)
    down_all = down_weight.reshape(EXPERTS, SHARD, FF_DEV, D)

    def one_expert(operands):
        rows, gate_up_part, down_part = operands
        total = jnp.zeros((N_EP * CAP, D), jnp.float32)
        for member in range(SHARD):
            hidden = jnp.dot(rows, gate_up_part[member], preferred_element_type=jnp.float32)
            gate_part = hidden[:, :FF_DEV]
            up_part = hidden[:, FF_DEV:]
            activated = ((up_part + 1.0) * gate_part * jax.nn.sigmoid(1.702 * gate_part)).astype(jnp.bfloat16)
            partial_value = jnp.dot(activated, down_part[member], preferred_element_type=jnp.float32).astype(jnp.bfloat16)
            total = total + partial_value.astype(jnp.float32)
        return total
    expert_sum = lax.map(one_expert, (buffer, gate_up_all, down_all))
    mixture = jnp.zeros((TOKENS, D), jnp.float32)
    for choice_k in range(TOP):
        picked = expert_sum[routes[:, choice_k], position[:, choice_k]]
        mixture = mixture + route_prob[:, choice_k:choice_k + 1] * picked
    return (stream + mixture).astype(jnp.bfloat16)
```

```python
import functools

import jax
import jax.numpy as jnp
from jax import lax
from jax.sharding import PartitionSpec as P

CHUNKS = 1


def route_weights(normed, routes, router_weight):
    experts = router_weight.shape[1]
    logits = jnp.dot(normed, router_weight, preferred_element_type=jnp.float32)
    expert_ids = lax.broadcasted_iota(jnp.int32, (1, 1, experts), 2)
    hits = jnp.any(routes[:, :, None] == expert_ids, axis=1)
    expo = jnp.where(hits, jnp.exp(logits), jnp.float32(0.0))
    return expo / jnp.sum(expo, axis=-1, keepdims=True)


def shards(tokens, routes, norm_gain, router_weight, gate_up_weight, down_weight):
    tok_rows, width = tokens.shape
    experts = router_weight.shape[1]
    devices = lax.axis_size("ep")
    shard_count = devices // experts
    ff_dev = down_weight.shape[1]
    stream = tokens.astype(jnp.float32)
    mean_square = jnp.mean(stream * stream, axis=-1, keepdims=True)
    normed = (stream * lax.rsqrt(mean_square + 1e-05) * norm_gain.astype(jnp.float32)).astype(
        jnp.bfloat16
    )
    weights = route_weights(normed, routes, router_weight)
    all_weights = lax.all_gather(weights, "ep", axis=0, tiled=False)
    expert = lax.axis_index("ep") // shard_count
    mine = lax.dynamic_slice_in_dim(all_weights, expert, 1, axis=2)
    rows = tok_rows // CHUNKS
    pieces = []
    for c in range(CHUNKS):
        part = lax.all_gather(normed[c * rows : (c + 1) * rows], "ep", axis=0, tiled=True)
        hidden = jnp.dot(part, gate_up_weight[0], preferred_element_type=jnp.float32)
        gate_part = hidden[:, :ff_dev]
        up_part = hidden[:, ff_dev:]
        scale = mine[:, c * rows : (c + 1) * rows].reshape(devices * rows, 1)
        activated = (
            (up_part + 1.0) * gate_part * jax.nn.sigmoid(1.702 * gate_part) * scale
        ).astype(jnp.bfloat16)
        partial_value = jnp.dot(
            activated, down_weight[0], preferred_element_type=jnp.float32
        ).astype(jnp.bfloat16)
        pieces.append(lax.psum_scatter(partial_value, "ep", scatter_dimension=0, tiled=True))
    mixture = jnp.concatenate(pieces, axis=0) if CHUNKS > 1 else pieces[0]
    return (stream + mixture.astype(jnp.float32)).astype(jnp.bfloat16)


def solution(mesh):
    in_specs = (
        P(("groups", "ep"), None),
        P(("groups", "ep"), None),
        P(),
        P(),
        P("ep", None, None),
        P("ep", None, None),
    )
    out_specs = P(("groups", "ep"), None)
    return jax.shard_map(shards, mesh=mesh, in_specs=in_specs, out_specs=out_specs, check_vma=False)
```

```python
import functools

import jax
import jax.numpy as jnp
from jax import lax
from jax.experimental import pallas as pl
from jax.experimental.pallas import tpu as pltpu
from jax.sharding import PartitionSpec as P

SHARD = 4
MESH = pl.DeviceIdType.MESH


def places(groups):
    me = lax.axis_index("ep")
    group = me // SHARD
    member = me % SHARD
    core = member % 2
    half = member // 2
    core_mate = me + 1 - 2 * core
    chip_mate = me + 2 - 4 * half
    return me, group, member, core, half, core_mate, chip_mate


def greet(groups, group, member, core_mate, chip_mate):
    barrier = pltpu.get_barrier_semaphore()
    others = [(group + r) % groups * SHARD + member for r in range(1, groups)]
    for other in [core_mate, chip_mate] + others:
        pl.semaphore_signal(barrier, inc=1, device_id={"ep": other}, device_id_type=MESH)
    pl.semaphore_wait(barrier, groups + 1)


def send(src, dst, sems, slot, device):
    return pltpu.make_async_remote_copy(
        src_ref=src,
        dst_ref=dst,
        send_sem=sems.at[0, slot],
        recv_sem=sems.at[1, slot],
        device_id={"ep": device},
        device_id_type=MESH,
    )


def dispatch_kernel(groups, buf, out, direct, across, paired, relayed, local):
    me, group, member, core, half, core_mate, chip_mate = places(groups)
    greet(groups, group, member, core_mate, chip_mate)
    own = pltpu.make_async_copy(buf.at[group], out.at[me], local)
    own.start()
    to_chip = [send(buf.at[group], out.at[me], across, 0, chip_mate)]
    to_chip[0].start()
    sent = []
    for r in range(1, groups):
        target = (group + r) % groups
        copy = send(buf.at[target], out.at[me], direct, r, target * SHARD + member)
        copy.start()
        sent.append(copy)
    to_core = [send(buf.at[group], out.at[me], paired, 0, core_mate)]
    to_core[0].start()
    for r in range(1, groups):
        source = (group + groups - r) % groups
        block = out.at[source * SHARD + member]
        sent[r - 1].wait_recv()
        for copies, sems, device in ((to_chip, across, chip_mate), (to_core, paired, core_mate)):
            copy = send(block, block, sems, r, device)
            copy.start()
            copies.append(copy)
    relays = []
    for r in range(groups):
        source = (group + groups - r) % groups
        block = out.at[source * SHARD + (member + 2) % SHARD]
        to_chip[r].wait_recv()
        copy = send(block, block, relayed, r, core_mate)
        copy.start()
        relays.append(copy)
    for r in range(groups):
        to_core[r].wait_recv()
        relays[r].wait_recv()
    own.wait()
    for copy in sent + to_chip + to_core + relays:
        copy.wait_send()


def dispatch(buffer, devices):
    groups, rows, width = buffer.shape
    sems = pltpu.SemaphoreType.DMA((2, groups))
    return pl.pallas_call(
        functools.partial(dispatch_kernel, groups),
        out_shape=jax.ShapeDtypeStruct((devices, rows, width), buffer.dtype),
        in_specs=[pl.BlockSpec(memory_space=pltpu.VMEM)],
        out_specs=pl.BlockSpec(memory_space=pl.ANY),
        scratch_shapes=[sems, sems, sems, sems, pltpu.SemaphoreType.DMA],
        compiler_params=pltpu.CompilerParams(collective_id=0, has_side_effects=True),
    )(buffer)


def collect_kernel(
    groups, part, out, got, summed, crossed, final, to_mate, to_chip, to_owner, local
):
    me, group, member, core, half, core_mate, chip_mate = places(groups)
    greet(groups, group, member, core_mate, chip_mate)
    order = [(group + r) % groups for r in range(groups)]
    pairs = []
    for step in range(2):
        side = (half + 1 + step) % 2
        for r in range(groups):
            slot = step * groups + r
            block = part.at[order[r] * SHARD + side * 2 + 1 - core]
            copy = send(block, got.at[slot], to_mate, slot, core_mate)
            copy.start()
            pairs.append(copy)

    def mate_sum(step, r):
        pairs[step * groups + r].wait_recv()
        side = (half + 1 + step) % 2
        mine = part[order[r] * SHARD + side * 2 + core].astype(jnp.float32)
        return mine + got[step * groups + r].astype(jnp.float32)

    crossing = [send(summed.at[r], crossed.at[r], to_chip, r, chip_mate) for r in range(groups)]
    for r in range(groups):
        summed[r] = mate_sum(0, r).astype(summed.dtype)
        if r > 0:
            crossing[r - 1].start()
    for r in range(groups):
        final[r] = mate_sum(1, r).astype(final.dtype)
        if r == 0:
            crossing[groups - 1].start()
    homing = [
        send(final.at[r], out.at[group], to_owner, r, order[r] * SHARD + member)
        for r in range(1, groups)
    ]
    own = pltpu.make_async_copy(final.at[0], out.at[group], local)
    for r in range(groups):
        crossing[r].wait_recv()
        total = final[r].astype(jnp.float32) + crossed[r].astype(jnp.float32)
        final[r] = total.astype(final.dtype)
        if r == 1:
            own.start()
        if r > 1:
            homing[r - 2].start()
    homing[groups - 2].start()
    for r in range(1, groups):
        homing[r - 1].wait_recv()
    own.wait()
    for copy in pairs + crossing + homing:
        copy.wait_send()


def collect(partial_value, groups):
    devices, rows, width = partial_value.shape
    dtype = partial_value.dtype
    return pl.pallas_call(
        functools.partial(collect_kernel, groups),
        out_shape=jax.ShapeDtypeStruct((groups, rows, width), dtype),
        in_specs=[pl.BlockSpec(memory_space=pltpu.VMEM)],
        out_specs=pl.BlockSpec(memory_space=pl.ANY),
        scratch_shapes=[
            pltpu.VMEM((2 * groups, rows, width), dtype),
            pltpu.VMEM((groups, rows, width), dtype),
            pltpu.VMEM((groups, rows, width), dtype),
            pltpu.VMEM((groups, rows, width), dtype),
            pltpu.SemaphoreType.DMA((2, 2 * groups)),
            pltpu.SemaphoreType.DMA((2, groups)),
            pltpu.SemaphoreType.DMA((2, groups)),
            pltpu.SemaphoreType.DMA,
        ],
        compiler_params=pltpu.CompilerParams(
            collective_id=1, has_side_effects=True, vmem_limit_bytes=60 * 1024 * 1024
        ),
    )(partial_value)


def shards(tokens, routes, norm_gain, router_weight, gate_up_weight, down_weight):
    tok_rows, width = tokens.shape
    top_count = routes.shape[1]
    experts = router_weight.shape[1]
    devices = lax.axis_size("ep")
    ff_dev = down_weight.shape[1]
    capacity = min(tok_rows, SHARD * (17 * tok_rows * top_count // (16 * experts * SHARD) + 1))
    capacity = -(-capacity // 8) * 8
    stream = tokens.astype(jnp.float32)
    mean_square = jnp.mean(stream * stream, axis=-1, keepdims=True)
    normed = (stream * lax.rsqrt(mean_square + 1e-05) * norm_gain.astype(jnp.float32)).astype(
        jnp.bfloat16
    )
    logits = jnp.dot(normed, router_weight, preferred_element_type=jnp.float32)
    expert_ids = lax.broadcasted_iota(jnp.int32, (1, 1, experts), 2)
    hits = jnp.any(routes[:, :, None] == expert_ids, axis=1)
    expo = jnp.where(hits, jnp.exp(logits), jnp.float32(0.0))
    prob = expo / jnp.sum(expo, axis=-1, keepdims=True)
    earlier = lax.broadcasted_iota(jnp.int32, (tok_rows, tok_rows), 1) < (
        lax.broadcasted_iota(jnp.int32, (tok_rows, tok_rows), 0)
    )
    rank = jnp.dot(
        earlier.astype(jnp.bfloat16),
        hits.astype(jnp.bfloat16),
        preferred_element_type=jnp.float32,
    ).astype(jnp.int32)
    slot = lax.broadcasted_iota(jnp.int32, (1, 1, capacity), 2)
    placed = (hits[:, :, None] & (rank[:, :, None] == slot)).reshape(tok_rows, experts * capacity)
    buffer = lax.dot_general(
        placed.astype(jnp.bfloat16),
        normed,
        (((0,), (0,)), ((), ())),
        preferred_element_type=jnp.float32,
    ).astype(jnp.bfloat16)
    received = dispatch(buffer.reshape(experts, capacity, width), devices)
    rows_in = received.reshape(devices * capacity, width)
    hidden = jnp.dot(rows_in, gate_up_weight[0], preferred_element_type=jnp.float32)
    gate_part = hidden[:, :ff_dev]
    up_part = hidden[:, ff_dev:]
    activated = ((up_part + 1.0) * gate_part * jax.nn.sigmoid(1.702 * gate_part)).astype(
        jnp.bfloat16
    )
    partial_value = jnp.dot(activated, down_weight[0], preferred_element_type=jnp.float32).astype(
        jnp.bfloat16
    )
    expert_sum = collect(partial_value.reshape(devices, capacity, width), experts)
    expert_sum = expert_sum.reshape(experts * capacity, width)
    spread = jnp.repeat(prob, capacity, axis=1) * placed.astype(jnp.float32)
    high = spread.astype(jnp.bfloat16)
    low = (spread - high.astype(jnp.float32)).astype(jnp.bfloat16)
    mixture = jnp.dot(high, expert_sum, preferred_element_type=jnp.float32) + jnp.dot(
        low, expert_sum, preferred_element_type=jnp.float32
    )
    return (stream + mixture).astype(jnp.bfloat16)


def solution(mesh):
    in_specs = (
        P(("groups", "ep"), None),
        P(("groups", "ep"), None),
        P(),
        P(),
        P("ep", None, None),
        P("ep", None, None),
    )
    out_specs = P(("groups", "ep"), None)
    return jax.shard_map(shards, mesh=mesh, in_specs=in_specs, out_specs=out_specs, check_vma=False)
```

```python
import functools

import jax
import jax.numpy as jnp
from jax import lax
from jax.experimental import pallas as pl
from jax.experimental.pallas import tpu as pltpu
from jax.sharding import PartitionSpec as P

SHARD = 4
MESH = pl.DeviceIdType.MESH


def places(groups):
    me = lax.axis_index("ep")
    group = me // SHARD
    member = me % SHARD
    core = member % 2
    half = member // 2
    core_mate = me + 1 - 2 * core
    chip_mate = me + 2 - 4 * half
    return me, group, member, core, half, core_mate, chip_mate


def greet(groups, group, member, core_mate, chip_mate):
    barrier = pltpu.get_barrier_semaphore()
    others = [(group + r) % groups * SHARD + member for r in range(1, groups)]
    for other in [core_mate, chip_mate] + others:
        pl.semaphore_signal(barrier, inc=1, device_id={"ep": other}, device_id_type=MESH)
    pl.semaphore_wait(barrier, groups + 1)


def send(src, dst, sems, slot, device):
    return pltpu.make_async_remote_copy(
        src_ref=src,
        dst_ref=dst,
        send_sem=sems.at[0, slot],
        recv_sem=sems.at[1, slot],
        device_id={"ep": device},
        device_id_type=MESH,
    )


def far_first(groups):
    return sorted(range(groups), key=lambda r: -min(r, groups - r))


def dispatch_kernel(groups, buf, out, direct, across, paired, relayed, local):
    me, group, member, core, half, core_mate, chip_mate = places(groups)
    greet(groups, group, member, core_mate, chip_mate)
    own = pltpu.make_async_copy(buf.at[group], out.at[me], local)
    own.start()
    to_chip = [send(buf.at[group], out.at[me], across, 0, chip_mate)]
    to_chip[0].start()
    turns = [1, groups - 1] + [r for r in far_first(groups) if 1 < r < groups - 1]
    sent = []
    for r in turns:
        target = (group + r) % groups
        copy = send(buf.at[target], out.at[me], direct, r, target * SHARD + member)
        copy.start()
        sent.append(copy)
    to_core = [send(buf.at[group], out.at[me], paired, 0, core_mate)]
    to_core[0].start()
    for at, r in enumerate(turns):
        source = (group + groups - r) % groups
        block = out.at[source * SHARD + member]
        sent[at].wait_recv()
        for copies, sems, device in ((to_chip, across, chip_mate), (to_core, paired, core_mate)):
            copy = send(block, block, sems, r, device)
            copy.start()
            copies.append(copy)
    relays = []
    for at, r in enumerate([0] + turns):
        source = (group + groups - r) % groups
        block = out.at[source * SHARD + (member + 2) % SHARD]
        to_chip[at].wait_recv()
        copy = send(block, block, relayed, r, core_mate)
        copy.start()
        relays.append(copy)
    for r in range(groups):
        to_core[r].wait_recv()
        relays[r].wait_recv()
    own.wait()
    for copy in sent + to_chip + to_core + relays:
        copy.wait_send()


def dispatch(buffer, devices):
    groups, rows, width = buffer.shape
    sems = pltpu.SemaphoreType.DMA((2, groups))
    return pl.pallas_call(
        functools.partial(dispatch_kernel, groups),
        out_shape=jax.ShapeDtypeStruct((devices, rows, width), buffer.dtype),
        in_specs=[pl.BlockSpec(memory_space=pltpu.VMEM)],
        out_specs=pl.BlockSpec(memory_space=pl.ANY),
        scratch_shapes=[sems, sems, sems, sems, pltpu.SemaphoreType.DMA],
        compiler_params=pltpu.CompilerParams(collective_id=0, has_side_effects=True),
    )(buffer)


def collect_kernel(
    groups, act, weight, out, part, got, summed, crossed, final, to_mate, to_chip, to_owner, local
):
    me, group, member, core, half, core_mate, chip_mate = places(groups)
    greet(groups, group, member, core_mate, chip_mate)
    rows = out.shape[1]
    chunk = SHARD * rows
    away = far_first(groups)
    owners = [(group + r) % groups for r in away]
    pairs = [
        [
            send(
                part.at[i, (half + 1 + side) % 2 * 2 + 1 - core],
                got.at[2 * i + side],
                to_mate,
                2 * i + side,
                core_mate,
            )
            for side in range(2)
        ]
        for i in range(groups)
    ]
    crossing = [send(summed.at[i], crossed.at[i], to_chip, i, chip_mate) for i in range(groups)]

    def mate_sum(i, side):
        pairs[i][side].wait_recv()
        mine = part[i, (half + 1 + side) % 2 * 2 + core].astype(jnp.float32)
        return (mine + got[2 * i + side].astype(jnp.float32)).astype(summed.dtype)

    for step in range(groups + 2):
        if step < groups:
            base = pl.multiple_of(owners[step] * chunk, chunk)
            value = jnp.dot(
                act[pl.ds(base, chunk), :], weight[...], preferred_element_type=jnp.float32
            )
            for j in range(SHARD):
                part[step, j] = value[j * rows : (j + 1) * rows].astype(part.dtype)
        if 1 <= step <= groups:
            for side in range(2):
                pairs[step - 1][side].start()
        if step >= 2:
            summed[step - 2] = mate_sum(step - 2, 0)
            final[step - 2] = mate_sum(step - 2, 1)
            crossing[step - 2].start()
    homing = [
        send(final.at[i], out.at[group], to_owner, away[i], owners[i] * SHARD + member)
        for i in range(groups - 1)
    ]
    own = pltpu.make_async_copy(final.at[groups - 1], out.at[group], local)
    for i in range(groups):
        crossing[i].wait_recv()
        total = final[i].astype(jnp.float32) + crossed[i].astype(jnp.float32)
        final[i] = total.astype(final.dtype)
        if i < groups - 1:
            homing[i].start()
        else:
            own.start()
    for copy in homing:
        copy.wait_recv()
    own.wait()
    for copy in [c for pair in pairs for c in pair] + crossing + homing:
        copy.wait_send()


def collect(activated, weight, groups, devices):
    rows = activated.shape[0] // devices
    width = weight.shape[1]
    dtype = weight.dtype
    return pl.pallas_call(
        functools.partial(collect_kernel, groups),
        out_shape=jax.ShapeDtypeStruct((groups, rows, width), dtype),
        in_specs=[pl.BlockSpec(memory_space=pltpu.VMEM)] * 2,
        out_specs=pl.BlockSpec(memory_space=pl.ANY),
        scratch_shapes=[
            pltpu.VMEM((groups, SHARD, rows, width), dtype),
            pltpu.VMEM((2 * groups, rows, width), dtype),
            pltpu.VMEM((groups, rows, width), dtype),
            pltpu.VMEM((groups, rows, width), dtype),
            pltpu.VMEM((groups, rows, width), dtype),
            pltpu.SemaphoreType.DMA((2, 2 * groups)),
            pltpu.SemaphoreType.DMA((2, groups)),
            pltpu.SemaphoreType.DMA((2, groups)),
            pltpu.SemaphoreType.DMA,
        ],
        compiler_params=pltpu.CompilerParams(
            collective_id=1, has_side_effects=True, vmem_limit_bytes=60 * 1024 * 1024
        ),
    )(activated, weight)


def shards(tokens, routes, norm_gain, router_weight, gate_up_weight, down_weight):
    tok_rows, width = tokens.shape
    top_count = routes.shape[1]
    experts = router_weight.shape[1]
    devices = lax.axis_size("ep")
    ff_dev = down_weight.shape[1]
    capacity = min(tok_rows, SHARD * (17 * tok_rows * top_count // (16 * experts * SHARD) + 1))
    capacity = -(-capacity // 8) * 8
    stream = tokens.astype(jnp.float32)
    mean_square = jnp.mean(stream * stream, axis=-1, keepdims=True)
    normed = (stream * lax.rsqrt(mean_square + 1e-05) * norm_gain.astype(jnp.float32)).astype(
        jnp.bfloat16
    )
    logits = jnp.dot(normed, router_weight, preferred_element_type=jnp.float32)
    expert_ids = lax.broadcasted_iota(jnp.int32, (1, 1, experts), 2)
    hits = jnp.any(routes[:, :, None] == expert_ids, axis=1)
    expo = jnp.where(hits, jnp.exp(logits), jnp.float32(0.0))
    prob = expo / jnp.sum(expo, axis=-1, keepdims=True)
    earlier = lax.broadcasted_iota(jnp.int32, (tok_rows, tok_rows), 1) < (
        lax.broadcasted_iota(jnp.int32, (tok_rows, tok_rows), 0)
    )
    rank = jnp.dot(
        earlier.astype(jnp.bfloat16),
        hits.astype(jnp.bfloat16),
        preferred_element_type=jnp.float32,
    ).astype(jnp.int32)
    slot = lax.broadcasted_iota(jnp.int32, (1, 1, capacity), 2)
    placed = (hits[:, :, None] & (rank[:, :, None] == slot)).reshape(tok_rows, experts * capacity)
    buffer = lax.dot_general(
        placed.astype(jnp.bfloat16),
        normed,
        (((0,), (0,)), ((), ())),
        preferred_element_type=jnp.float32,
    ).astype(jnp.bfloat16)
    received = dispatch(buffer.reshape(experts, capacity, width), devices)
    rows_in = received.reshape(devices * capacity, width)
    hidden = jnp.dot(rows_in, gate_up_weight[0], preferred_element_type=jnp.float32)
    gate_part = hidden[:, :ff_dev]
    up_part = hidden[:, ff_dev:]
    activated = ((up_part + 1.0) * gate_part * jax.nn.sigmoid(1.702 * gate_part)).astype(
        jnp.bfloat16
    )
    expert_sum = collect(activated, down_weight[0], experts, devices)
    expert_sum = expert_sum.reshape(experts * capacity, width)
    spread = jnp.repeat(prob, capacity, axis=1) * placed.astype(jnp.float32)
    high = spread.astype(jnp.bfloat16)
    low = (spread - high.astype(jnp.float32)).astype(jnp.bfloat16)
    mixture = jnp.dot(high, expert_sum, preferred_element_type=jnp.float32) + jnp.dot(
        low, expert_sum, preferred_element_type=jnp.float32
    )
    return (stream + mixture).astype(jnp.bfloat16)


def solution(mesh):
    in_specs = (
        P(("groups", "ep"), None),
        P(("groups", "ep"), None),
        P(),
        P(),
        P("ep", None, None),
        P("ep", None, None),
    )
    out_specs = P(("groups", "ep"), None)
    return jax.shard_map(shards, mesh=mesh, in_specs=in_specs, out_specs=out_specs, check_vma=False)
```

```python
import functools

import jax
import jax.numpy as jnp
from jax import lax
from jax.experimental import pallas as pl
from jax.experimental.pallas import tpu as pltpu
from jax.sharding import PartitionSpec as P

SHARD = 4
MESH = pl.DeviceIdType.MESH


def places(groups):
    me = lax.axis_index("ep")
    group = me // SHARD
    member = me % SHARD
    core = member % 2
    half = member // 2
    core_mate = me + 1 - 2 * core
    chip_mate = me + 2 - 4 * half
    return me, group, member, core, half, core_mate, chip_mate


def greet(groups, group, member, core_mate, chip_mate):
    barrier = pltpu.get_barrier_semaphore()
    others = [(group + r) % groups * SHARD + member for r in range(1, groups)]
    for other in [core_mate, chip_mate] + others:
        pl.semaphore_signal(barrier, inc=1, device_id={"ep": other}, device_id_type=MESH)
    pl.semaphore_wait(barrier, groups + 1)


def send(src, dst, sems, slot, device):
    return pltpu.make_async_remote_copy(
        src_ref=src,
        dst_ref=dst,
        send_sem=sems.at[0, slot],
        recv_sem=sems.at[1, slot],
        device_id={"ep": device},
        device_id_type=MESH,
    )


def far_first(groups):
    return sorted(range(groups), key=lambda r: -min(r, groups - r))


def dispatch_kernel(groups, buf, out, direct, across, paired, relayed, local):
    me, group, member, core, half, core_mate, chip_mate = places(groups)
    greet(groups, group, member, core_mate, chip_mate)
    own = pltpu.make_async_copy(buf.at[group], out.at[me], local)
    own.start()
    to_chip = [send(buf.at[group], out.at[me], across, 0, chip_mate)]
    to_chip[0].start()
    turns = list(range(1, groups))
    sent = []
    for r in turns:
        target = (group + r) % groups
        copy = send(buf.at[target], out.at[me], direct, r, target * SHARD + member)
        copy.start()
        sent.append(copy)
    to_core = [send(buf.at[group], out.at[me], paired, 0, core_mate)]
    to_core[0].start()
    for at, r in enumerate(turns):
        source = (group + groups - r) % groups
        block = out.at[source * SHARD + member]
        sent[at].wait_recv()
        for copies, sems, device in ((to_chip, across, chip_mate), (to_core, paired, core_mate)):
            copy = send(block, block, sems, r, device)
            copy.start()
            copies.append(copy)
    relays = []
    for at, r in enumerate([0] + turns):
        source = (group + groups - r) % groups
        block = out.at[source * SHARD + (member + 2) % SHARD]
        to_chip[at].wait_recv()
        copy = send(block, block, relayed, r, core_mate)
        copy.start()
        relays.append(copy)
    for r in range(groups):
        to_core[r].wait_recv()
        relays[r].wait_recv()
    own.wait()
    for copy in sent + to_chip + to_core + relays:
        copy.wait_send()


def dispatch(buffer, devices):
    groups, rows, width = buffer.shape
    sems = pltpu.SemaphoreType.DMA((2, groups))
    return pl.pallas_call(
        functools.partial(dispatch_kernel, groups),
        out_shape=jax.ShapeDtypeStruct((devices, rows, width), buffer.dtype),
        in_specs=[pl.BlockSpec(memory_space=pltpu.VMEM)],
        out_specs=pl.BlockSpec(memory_space=pl.ANY),
        scratch_shapes=[sems, sems, sems, sems, pltpu.SemaphoreType.DMA],
        compiler_params=pltpu.CompilerParams(collective_id=0, has_side_effects=True),
    )(buffer)


def collect_kernel(
    groups, act, weight, out, part, got, summed, crossed, final, to_mate, to_chip, to_owner, local
):
    me, group, member, core, half, core_mate, chip_mate = places(groups)
    greet(groups, group, member, core_mate, chip_mate)
    rows = out.shape[1]
    chunk = SHARD * rows
    away = far_first(groups)
    owners = [(group + r) % groups for r in away]
    pairs = [
        [
            send(
                part.at[i, (half + 1 + side) % 2 * 2 + 1 - core],
                got.at[2 * i + side],
                to_mate,
                2 * i + side,
                core_mate,
            )
            for side in range(2)
        ]
        for i in range(groups)
    ]
    crossing = [send(summed.at[i], crossed.at[i], to_chip, i, chip_mate) for i in range(groups)]

    def mate_sum(i, side):
        pairs[i][side].wait_recv()
        mine = part[i, (half + 1 + side) % 2 * 2 + core].astype(jnp.float32)
        return (mine + got[2 * i + side].astype(jnp.float32)).astype(summed.dtype)

    for step in range(groups + 2):
        if step < groups:
            base = pl.multiple_of(owners[step] * chunk, chunk)
            value = jnp.dot(
                act[pl.ds(base, chunk), :], weight[...], preferred_element_type=jnp.float32
            )
            for j in range(SHARD):
                part[step, j] = value[j * rows : (j + 1) * rows].astype(part.dtype)
        if 1 <= step <= groups:
            for side in range(2):
                pairs[step - 1][side].start()
        if step >= 2:
            summed[step - 2] = mate_sum(step - 2, 0)
            final[step - 2] = mate_sum(step - 2, 1)
            crossing[step - 2].start()
    homing = [
        send(final.at[i], out.at[group], to_owner, away[i], owners[i] * SHARD + member)
        for i in range(groups - 1)
    ]
    own = pltpu.make_async_copy(final.at[groups - 1], out.at[group], local)
    for i in range(groups):
        crossing[i].wait_recv()
        total = final[i].astype(jnp.float32) + crossed[i].astype(jnp.float32)
        final[i] = total.astype(final.dtype)
        if i < groups - 1:
            homing[i].start()
        else:
            own.start()
    for copy in homing:
        copy.wait_recv()
    own.wait()
    for copy in [c for pair in pairs for c in pair] + crossing + homing:
        copy.wait_send()


def collect(activated, weight, groups, devices):
    rows = activated.shape[0] // devices
    width = weight.shape[1]
    dtype = weight.dtype
    return pl.pallas_call(
        functools.partial(collect_kernel, groups),
        out_shape=jax.ShapeDtypeStruct((groups, rows, width), dtype),
        in_specs=[pl.BlockSpec(memory_space=pltpu.VMEM)] * 2,
        out_specs=pl.BlockSpec(memory_space=pl.ANY),
        scratch_shapes=[
            pltpu.VMEM((groups, SHARD, rows, width), dtype),
            pltpu.VMEM((2 * groups, rows, width), dtype),
            pltpu.VMEM((groups, rows, width), dtype),
            pltpu.VMEM((groups, rows, width), dtype),
            pltpu.VMEM((groups, rows, width), dtype),
            pltpu.SemaphoreType.DMA((2, 2 * groups)),
            pltpu.SemaphoreType.DMA((2, groups)),
            pltpu.SemaphoreType.DMA((2, groups)),
            pltpu.SemaphoreType.DMA,
        ],
        compiler_params=pltpu.CompilerParams(
            collective_id=1, has_side_effects=True, vmem_limit_bytes=60 * 1024 * 1024
        ),
    )(activated, weight)


def shards(tokens, routes, norm_gain, router_weight, gate_up_weight, down_weight):
    tok_rows, width = tokens.shape
    top_count = routes.shape[1]
    experts = router_weight.shape[1]
    devices = lax.axis_size("ep")
    ff_dev = down_weight.shape[1]
    capacity = min(tok_rows, SHARD * (17 * tok_rows * top_count // (16 * experts * SHARD) + 1))
    capacity = -(-capacity // 8) * 8
    stream = tokens.astype(jnp.float32)
    mean_square = jnp.mean(stream * stream, axis=-1, keepdims=True)
    normed = (stream * lax.rsqrt(mean_square + 1e-05) * norm_gain.astype(jnp.float32)).astype(
        jnp.bfloat16
    )
    logits = jnp.dot(normed, router_weight, preferred_element_type=jnp.float32)
    expert_ids = lax.broadcasted_iota(jnp.int32, (1, 1, experts), 2)
    hits = jnp.any(routes[:, :, None] == expert_ids, axis=1)
    expo = jnp.where(hits, jnp.exp(logits), jnp.float32(0.0))
    prob = expo / jnp.sum(expo, axis=-1, keepdims=True)
    earlier = lax.broadcasted_iota(jnp.int32, (tok_rows, tok_rows), 1) < (
        lax.broadcasted_iota(jnp.int32, (tok_rows, tok_rows), 0)
    )
    rank = jnp.dot(
        earlier.astype(jnp.bfloat16),
        hits.astype(jnp.bfloat16),
        preferred_element_type=jnp.float32,
    ).astype(jnp.int32)
    slot = lax.broadcasted_iota(jnp.int32, (1, 1, capacity), 2)
    placed = (hits[:, :, None] & (rank[:, :, None] == slot)).reshape(tok_rows, experts * capacity)
    buffer = lax.dot_general(
        placed.astype(jnp.bfloat16),
        normed,
        (((0,), (0,)), ((), ())),
        preferred_element_type=jnp.float32,
    ).astype(jnp.bfloat16)
    received = dispatch(buffer.reshape(experts, capacity, width), devices)
    rows_in = received.reshape(devices * capacity, width)
    hidden = jnp.dot(rows_in, gate_up_weight[0], preferred_element_type=jnp.float32)
    gate_part = hidden[:, :ff_dev]
    up_part = hidden[:, ff_dev:]
    activated = ((up_part + 1.0) * gate_part * jax.nn.sigmoid(1.702 * gate_part)).astype(
        jnp.bfloat16
    )
    expert_sum = collect(activated, down_weight[0], experts, devices)
    expert_sum = expert_sum.reshape(experts * capacity, width)
    spread = jnp.repeat(prob, capacity, axis=1) * placed.astype(jnp.float32)
    high = spread.astype(jnp.bfloat16)
    low = (spread - high.astype(jnp.float32)).astype(jnp.bfloat16)
    mixture = jnp.dot(high, expert_sum, preferred_element_type=jnp.float32) + jnp.dot(
        low, expert_sum, preferred_element_type=jnp.float32
    )
    return (stream + mixture).astype(jnp.bfloat16)


def solution(mesh):
    in_specs = (
        P(("groups", "ep"), None),
        P(("groups", "ep"), None),
        P(),
        P(),
        P("ep", None, None),
        P("ep", None, None),
    )
    out_specs = P(("groups", "ep"), None)
    return jax.shard_map(shards, mesh=mesh, in_specs=in_specs, out_specs=out_specs, check_vma=False)
```
